32 devices in a mesh: rep: 1 (over z), data: 4 (over y), model: 8 (over x, core).
Axes of the slice: x: 4, y: 4, z: 1, core: 2. Of those that a mesh axis runs over, the one named last changes fastest.
The devices are a block of a 4x4x8 slice.
Arguments:
- x_in: bfloat16 [8, 1024, 4096], P(('rep', 'data'), 'model')
- key_lens: int32 [8], P(('rep', 'data'))
- ln_gain: bfloat16 [2, 4096], P(None, 'data')
- w_in: bfloat16 [2, 4096, 40960], P(None, 'data', 'model')
- w_out_attn: bfloat16 [2, 4096, 4096], P(None, 'model', 'data')
- w_out_mlp: bfloat16 [2, 16384, 4096], P(None, 'model', 'data')
Outputs:
- output: bfloat16 [8, 1024, 4096], P(('rep', 'data'), 'model')
All inputs are finite; a program needn't handle non-finite values.
Results may differ from the reference program's by a relative error of at most 0.0171323.
Values are sent between devices in bfloat16 or wider.
A program may use at most 768 MiB of HBM per device.

```python
import jax
import jax.numpy as jnp
from jax import lax

D = 4096
HEADS = 16
HEAD = 256
FF = 16384
KV_HEADS = 8
LAYERS = 2
BATCH = 8
SEQ = 1024

Q_GROUP = HEADS // KV_HEADS
FF_GROUP = FF // KV_HEADS
Q_WIDTH = Q_GROUP * HEAD
FF_START = Q_WIDTH + 2 * HEAD
BLOCK_IN = FF_START + 2 * FF_GROUP
EPSILON = 1e-6
NEG_BIG = -1e30


def draw_lengths(len_key):
    drawn = jax.random.randint(len_key, (BATCH,), SEQ // 2, SEQ + 1, dtype=jnp.int32)
    return jnp.where(jnp.arange(BATCH) == 0, SEQ, drawn).astype(jnp.int32)


def setup_inputs(seed: int = 0, part: int = 0) -> dict:
    part_key = jax.random.fold_in(jax.random.key(seed), part)
    act_key, len_key = jax.random.split(part_key, 2)
    shared = jax.random.split(jax.random.key(seed + 1), 4)
    x_in = jax.random.normal(act_key, (BATCH, SEQ, D), jnp.float32).astype(jnp.bfloat16)
    key_lens = draw_lengths(len_key)
    ln_gain = (1.0 + 0.3 * jax.random.normal(shared[0], (LAYERS, D), jnp.float32)).astype(jnp.bfloat16)
    in_cols = jnp.arange(BLOCK_IN)
    in_scale = jnp.where(in_cols < Q_WIDTH + HEAD, 1.5, 1.0) * D ** -0.5
    w_in = (jax.random.normal(shared[1], (LAYERS, D, KV_HEADS, BLOCK_IN), jnp.float32) * in_scale).reshape(LAYERS, D, KV_HEADS * BLOCK_IN).astype(jnp.bfloat16)
    out_scale = (HEADS * HEAD + FF) ** -0.5
    w_out_attn = (2.0 * out_scale * jax.random.normal(shared[2], (LAYERS, HEADS * HEAD, D), jnp.float32)).astype(jnp.bfloat16)
    w_out_mlp = (out_scale * jax.random.normal(shared[3], (LAYERS, FF, D), jnp.float32)).astype(jnp.bfloat16)
    return {'x_in': x_in, 'key_lens': key_lens, 'ln_gain': ln_gain, 'w_in': w_in, 'w_out_attn': w_out_attn, 'w_out_mlp': w_out_mlp}


def layer_norm(act_in, gain_vec):
    act_f32 = act_in.astype(jnp.float32)
    row_mean = jnp.mean(act_f32, axis=-1, keepdims=True)
    centered = act_f32 - row_mean
    row_var = jnp.mean(centered * centered, axis=-1, keepdims=True)
    return (centered * lax.rsqrt(row_var + EPSILON) * gain_vec.astype(jnp.float32)).astype(jnp.bfloat16)


def mix_block(h_seq, key_len, w_in_l, w_attn_g, w_mlp_g):
    projected = jnp.dot(h_seq, w_in_l, preferred_element_type=jnp.float32).astype(jnp.bfloat16)
    projected = projected.reshape(SEQ, KV_HEADS, BLOCK_IN).astype(jnp.float32)
    queries = projected[:, :, :Q_WIDTH].reshape(SEQ, KV_HEADS, Q_GROUP, HEAD)
    key_heads = projected[:, :, Q_WIDTH:Q_WIDTH + HEAD]
    value_heads = projected[:, :, Q_WIDTH + HEAD:FF_START]
    gate_proj = projected[:, :, FF_START:FF_START + FF_GROUP]
    up_proj = projected[:, :, FF_START + FF_GROUP:]
    scores = jnp.einsum('qhgd,khd->hgqk', queries, key_heads) * HEAD ** -0.5
    positions = jnp.arange(SEQ)
    allowed = (positions[None, :] <= positions[:, None]) & (positions[None, :] < key_len)
    scores = jnp.where(allowed, scores, NEG_BIG)
    soft_probs = jax.nn.softmax(scores, axis=-1)
    attn_heads = jnp.einsum('hgqk,khd->qhgd', soft_probs, value_heads).astype(jnp.bfloat16).reshape(SEQ, KV_HEADS, Q_WIDTH)
    mlp_act = (jax.nn.silu(gate_proj) * up_proj).astype(jnp.bfloat16)
    group_part = (jnp.einsum('shr,hrd->hsd', attn_heads.astype(jnp.float32), w_attn_g) + jnp.einsum('shf,hfd->hsd', mlp_act.astype(jnp.float32), w_mlp_g)).astype(jnp.bfloat16)
    return jnp.sum(group_part.astype(jnp.float32), axis=0)


def reference(x_in, key_lens, ln_gain, w_in, w_out_attn, w_out_mlp):
    def layer_step(hidden, layer_weights):
        gain_vec, w_in_l, w_attn_l, w_mlp_l = layer_weights
        w_attn_g = w_attn_l.reshape(KV_HEADS, Q_WIDTH, D).astype(jnp.float32)
        w_mlp_g = w_mlp_l.reshape(KV_HEADS, FF_GROUP, D).astype(jnp.float32)

        def per_sequence(seq_args):
            x_seq, key_len = seq_args
            h_seq = layer_norm(x_seq, gain_vec)
            z_sum = mix_block(h_seq, key_len, w_in_l, w_attn_g, w_mlp_g)
            return (x_seq.astype(jnp.float32) + z_sum).astype(jnp.bfloat16)

        return lax.map(per_sequence, (hidden, key_lens)), None

    y_out, unused_stack = lax.scan(layer_step, x_in, (ln_gain, w_in, w_out_attn, w_out_mlp))
    return y_out
```

```python
import jax
import jax.numpy as jnp
from jax import lax
from jax.experimental import pallas as pl
from jax.experimental.pallas import tpu as pltpu
from jax.sharding import PartitionSpec as P


EPSILON = 1e-6
BOTH = ('data', 'model')


def layer_norm(act_in, gain_vec):
    act_f32 = act_in.astype(jnp.float32)
    row_mean = jnp.mean(act_f32, axis=-1, keepdims=True)
    centered = act_f32 - row_mean
    row_var = jnp.mean(centered * centered, axis=-1, keepdims=True)
    return (centered * lax.rsqrt(row_var + EPSILON) * gain_vec.astype(jnp.float32)).astype(jnp.bfloat16)


def matmul(lhs, rhs):
    return jnp.dot(lhs, rhs, preferred_element_type=jnp.float32)


def project(h_seq, slab_ids, ours, theirs, total_in, final):
    n_slabs = len(ours)
    rows, cols = h_seq.shape[0], ours[0].shape[1]
    depth = ours[0].shape[0]
    tile, chunk = 512, 512
    tiles = cols // tile
    out_dtype = jnp.bfloat16 if final else jnp.float32

    def kernel(ids_ref, *refs):
        h_refs, w_refs, rest = refs[:n_slabs], refs[n_slabs:3 * n_slabs], refs[3 * n_slabs:]

        def run(w_half):
            @pl.loop(0, rows // chunk)
            def _(step):
                at = pl.ds(pl.multiple_of(step * chunk, chunk), chunk)
                total = matmul(h_refs[0][at, :], w_half[0][...])
                for h_ref, w_ref in zip(h_refs[1:], w_half[1:]):
                    total = total + matmul(h_ref[at, :], w_ref[...])
                if len(rest) == 2:
                    total = total + rest[0][0, at, :]
                rest[-1][0, at, :] = total.astype(out_dtype)

        @pl.when(pl.program_id(0) == 0)
        def _():
            run(w_refs[:n_slabs])

        @pl.when(pl.program_id(0) == 1)
        def _():
            run(w_refs[n_slabs:])

    in_specs = [pl.BlockSpec((rows, depth), lambda p, n, ids, i=i: (0, ids[i])) for i in range(n_slabs)]
    in_specs += [pl.BlockSpec((depth, tile), lambda p, n, ids: (0, jnp.where(p == 0, n, tiles - 1)))] * n_slabs
    in_specs += [pl.BlockSpec((depth, tile), lambda p, n, ids: (0, jnp.where(p == 0, 0, n)))] * n_slabs
    wide = pl.BlockSpec((1, rows, tile), lambda p, n, ids: (p, 0, n))
    args = [h_seq] * n_slabs + list(ours) + list(theirs)
    if total_in is not None:
        in_specs.append(wide)
        args.append(total_in)
    out_shape = jax.ShapeDtypeStruct((2, rows, cols), out_dtype)
    flops = 2 * 2 * n_slabs * rows * depth * cols
    return pl.pallas_call(
        kernel,
        out_shape=out_shape,
        grid_spec=pltpu.PrefetchScalarGridSpec(num_scalar_prefetch=1, grid=(2, tiles), in_specs=in_specs, out_specs=wide),
        cost_estimate=pl.CostEstimate(flops=flops, bytes_accessed=2 * n_slabs * depth * (rows + 2 * cols) + 4 * rows * cols, transcendentals=0),
    )(jnp.stack(slab_ids).astype(jnp.int32), *args)


def mix_out(attn, mlp, w_ours, w_theirs):
    n_seq = len(attn)
    _, rows, q_cut = attn[0].shape
    ff = mlp[0].shape[2]
    cols = w_ours.shape[1]
    chunk = 512
    steps = rows // chunk

    def kernel(*refs):
        lhs, (wa_ref, wb_ref, out_ref) = refs[:-3], refs[-3:]

        def run(a_ref, m_ref):
            total = matmul(a_ref[0], wa_ref[:q_cut, :]) + matmul(m_ref[0], wa_ref[q_cut:, :])
            total = total + matmul(a_ref[1], wb_ref[:q_cut, :]) + matmul(m_ref[1], wb_ref[q_cut:, :])
            out_ref[0] = total.astype(jnp.bfloat16)

        for b in range(n_seq):
            @pl.when(pl.program_id(0) == b)
            def _(b=b):
                run(lhs[2 * b], lhs[2 * b + 1])

    in_specs, args = [], []
    for b in range(n_seq):
        for arr in (attn[b], mlp[b]):
            in_specs.append(pl.BlockSpec((2, chunk, arr.shape[2]), lambda s, m, b=b: (0, jnp.where(s == b, m, jnp.where(s < b, 0, steps - 1)), 0)))
            args.append(arr)
    in_specs += [pl.BlockSpec(w_ours.shape, lambda s, m: (0, 0))] * 2
    return pl.pallas_call(
        kernel,
        out_shape=jax.ShapeDtypeStruct((n_seq, rows, cols), jnp.bfloat16),
        grid=(n_seq, steps),
        in_specs=in_specs,
        out_specs=pl.BlockSpec((1, chunk, cols), lambda s, m: (s, m, 0)),
        cost_estimate=pl.CostEstimate(flops=4 * n_seq * rows * (q_cut + ff) * cols, bytes_accessed=4 * n_seq * rows * (q_cut + ff) + 4 * w_ours.size + 2 * n_seq * rows * cols, transcendentals=0),
    )(*args, w_ours, w_theirs)


def attend(both, core, key_len, head_dim):
    _, rows, _ = both.shape
    chunk = 256

    def kernel(nums_ref, q_ref, k_ref, v_ref, out_ref):
        start = pl.program_id(1) * chunk
        scores = lax.dot_general(q_ref[0], k_ref[0], (((1,), (1,)), ((), ())), preferred_element_type=jnp.float32) * head_dim ** -0.5
        q_pos = start + lax.broadcasted_iota(jnp.int32, scores.shape, 0)
        k_pos = lax.broadcasted_iota(jnp.int32, scores.shape, 1)
        scores = jnp.where((k_pos <= q_pos) & (k_pos < nums_ref[1]), scores, -1e30)
        weights = jnp.exp(scores - jnp.max(scores, axis=-1, keepdims=True))
        norm = jnp.sum(weights, axis=-1, keepdims=True)
        probs = weights / norm
        out = jnp.dot(probs, v_ref[0].astype(jnp.float32), preferred_element_type=jnp.float32)
        out_ref[0] = out.astype(jnp.bfloat16)

    return pl.pallas_call(
        kernel,
        out_shape=jax.ShapeDtypeStruct((2, rows, head_dim), jnp.bfloat16),
        grid_spec=pltpu.PrefetchScalarGridSpec(
            num_scalar_prefetch=1,
            grid=(2, rows // chunk),
            in_specs=[
                pl.BlockSpec((1, chunk, head_dim), lambda j, m, nums: (j, m, 0)),
                pl.BlockSpec((1, rows, head_dim), lambda j, m, nums: (nums[0], 0, 1)),
                pl.BlockSpec((1, rows, head_dim), lambda j, m, nums: (1 - nums[0], 0, 1)),
            ],
            out_specs=pl.BlockSpec((1, chunk, head_dim), lambda j, m, nums: (j, m, 0)),
        ),
        cost_estimate=pl.CostEstimate(flops=8 * rows * rows * head_dim, bytes_accessed=16 * rows * head_dim, transcendentals=2 * rows * rows),
    )(jnp.stack([core, key_len]).astype(jnp.int32), both, both, both)


def split_columns(w_in, layer_idx, core, head_dim, q_group, ff_half):
    _, rows, width = w_in.shape
    tile = head_dim
    ff_tiles = ff_half // tile
    n_tiles = width // tile // 2

    def source(n, j):
        gate = q_group + 2 + j * ff_tiles + (n - 2)
        up = q_group + 2 + 2 * ff_tiles + j * ff_tiles + (n - 2 - ff_tiles)
        return jnp.where(n == 0, j, jnp.where(n == 1, q_group + j, jnp.where(n < 2 + ff_tiles, gate, up)))

    def kernel(core_ref, own_ref, other_ref, own_out, other_out):
        own_out[...] = own_ref[0]
        other_out[...] = other_ref[0]

    out = pl.BlockSpec((rows, tile), lambda n, c: (0, n))
    return pl.pallas_call(
        kernel,
        out_shape=[jax.ShapeDtypeStruct((rows, width // 2), w_in.dtype)] * 2,
        grid_spec=pltpu.PrefetchScalarGridSpec(
            num_scalar_prefetch=1,
            grid=(n_tiles,),
            in_specs=[
                pl.BlockSpec((1, rows, tile), lambda n, c: (layer_idx, 0, source(n, c[0]))),
                pl.BlockSpec((1, rows, tile), lambda n, c: (layer_idx, 0, source(n, 1 - c[0]))),
            ],
            out_specs=[out, out],
        ),
        cost_estimate=pl.CostEstimate(flops=rows * width * 8, bytes_accessed=4 * rows * width, transcendentals=0),
    )(core.reshape(1).astype(jnp.int32), w_in, w_in)


def split_rows(w_attn, w_mlp, layer_idx, core):
    _, q_rows, cols = w_attn.shape
    ff = w_mlp.shape[1]
    q_half, ff_half = q_rows // 2, ff // 2
    tile = q_half
    n_tiles = 1 + ff_half // tile

    def kernel(core_ref, own_a, own_m, other_a, other_m, own_out, other_out):
        @pl.when(pl.program_id(0) == 0)
        def _():
            own_out[...] = own_a[0]
            other_out[...] = other_a[0]

        @pl.when(pl.program_id(0) > 0)
        def _():
            own_out[...] = own_m[0]
            other_out[...] = other_m[0]

    def a_spec(flip):
        return pl.BlockSpec((1, tile, cols), lambda n, c: (layer_idx, 1 - c[0] if flip else c[0], 0))

    def m_spec(flip):
        return pl.BlockSpec((1, tile, cols), lambda n, c: (layer_idx, (1 - c[0] if flip else c[0]) * (ff_half // tile) + jnp.maximum(n - 1, 0), 0))

    out = pl.BlockSpec((tile, cols), lambda n, c: (n, 0))
    return pl.pallas_call(
        kernel,
        out_shape=[jax.ShapeDtypeStruct((q_half + ff_half, cols), w_attn.dtype)] * 2,
        grid_spec=pltpu.PrefetchScalarGridSpec(
            num_scalar_prefetch=1,
            grid=(n_tiles,),
            in_specs=[a_spec(False), m_spec(False), a_spec(True), m_spec(True)],
            out_specs=[out, out],
        ),
        cost_estimate=pl.CostEstimate(flops=(q_rows + ff) * cols * 8, bytes_accessed=4 * (q_rows + ff) * cols, transcendentals=0),
    )(core.reshape(1).astype(jnp.int32), w_attn, w_mlp, w_attn, w_mlp)


def solution(mesh):
    n_data, n_model = mesh.shape['data'], mesh.shape['model']
    batch_axes = ('rep', 'data')
    last = n_data - 1

    def table(move):
        pairs = []
        for row in range(n_data):
            for col in range(n_model):
                to = move(row, col)
                if to is not None:
                    pairs.append((row * n_model + col, to[0] * n_model + to[1]))
        return pairs

    core_swap = table(lambda r, m: (r, m ^ 1))
    near_swap = table(lambda r, m: (r ^ 1, m))
    far_swap = table(lambda r, m: (last - r, m))
    spread_a = table(lambda r, m: (r ^ 1, m ^ 1) if m % 2 == 0 else (r, m ^ 1))
    spread_b = table(lambda r, m: None if m % 2 == 0 else (r ^ 1, m))
    collect_a = table(lambda r, m: (r, m ^ 1) if m % 2 == 0 else (r ^ 1, m ^ 1))
    lanes = [list(range(0, n_model, 2)), list(range(1, n_model, 2))]

    def send(val, pairs):
        return lax.ppermute(val, BOTH, pairs)

    def two_layers(x_loc, len_loc, gain_loc, w_in_loc, w_attn_loc, w_mlp_loc):
        n_layers, slab, block_in = w_in_loc.shape
        attn_width = w_attn_loc.shape[1]
        ff_local = w_mlp_loc.shape[1]
        head_dim = (block_in - attn_width - 2 * ff_local) // 2
        q_group = attn_width // head_dim
        batch_loc, seq_loc = x_loc.shape[0], x_loc.shape[1]
        ff_half = ff_local // 2
        row = lax.axis_index('data')
        core = lax.rem(lax.axis_index('model'), 2)
        even = core == 0
        wanted = lax.rem((row + 1) // 2, 2)
        mine_wanted = wanted == core
        slabs = (row, row ^ 1, last - row, (last - row) ^ 1)

        work_lens = jnp.where(even, len_loc, send(len_loc, near_swap))
        gain_all = lax.all_gather(gain_loc, 'data', axis=1, tiled=True)

        def pieces(keep_half, give_half):
            other = send(give_half, core_swap)
            keep = jnp.where(mine_wanted, keep_half, other)
            give = jnp.where(mine_wanted, other, keep_half)
            near = send(give, near_swap)
            far = send(keep, far_swap)
            far_near = send(near, far_swap)
            ours = (keep, near, far, far_near)
            theirs = tuple(send(p, core_swap) for p in ours)
            return ours, theirs

        hidden = x_loc
        w_pieces = []
        for layer_idx in range(n_layers):
            ins = pieces(*split_columns(w_in_loc, layer_idx, core, head_dim, q_group, ff_half))
            outs = pieces(*split_rows(w_attn_loc, w_mlp_loc, layer_idx, core))
            w_pieces.append((ins, outs))

        for layer_idx in range(n_layers):
            ins, outs = w_pieces[layer_idx]
            normed = layer_norm(hidden, gain_all[layer_idx])
            h_seqs = []
            for b in range(batch_loc):
                got_a = send(normed[b], spread_a)
                got_b = send(normed[b], spread_b)
                pair = jnp.concatenate([jnp.where(even, normed[b], got_a), jnp.where(even, got_a, got_b)], axis=0)
                h_seqs.append(lax.all_gather(pair, 'model', axis=0, tiled=True, axis_index_groups=lanes))
            firsts_in, totals = (ins[0][:3], ins[1][:3]), []
            for b in range(batch_loc):
                totals.append(project(h_seqs[b], slabs[:3], *firsts_in, None, False))
            attn_all, mlp_all = [], []
            for b in range(batch_loc):
                both = project(h_seqs[b], slabs[3:], ins[0][3:], ins[1][3:], totals[b], True)
                ff_at = attn_width // 2 + head_dim
                attn_all.append(attend(both, core, work_lens[b], head_dim))
                gate, up = both[:, :, ff_at:ff_at + ff_half], both[:, :, ff_at + ff_half:]
                mlp_all.append((jax.nn.silu(gate.astype(jnp.float32)) * up.astype(jnp.float32)).astype(jnp.bfloat16))
            firsts, seconds = [], []
            for i in range(n_data):
                part = mix_out(attn_all, mlp_all, outs[0][i], outs[1][i])
                pair = lax.psum_scatter(part, 'model', scatter_dimension=1, tiled=True, axis_index_groups=lanes)
                firsts.append(pair[:, :seq_loc])
                seconds.append(pair[:, seq_loc:])
            z_slabs = []
            for i in range(n_data):
                got_a = send(jnp.where(even, seconds[i], firsts[i ^ 1]), collect_a)
                got_b = send(seconds[i ^ 1], spread_b)
                z_slabs.append(jnp.where(even, firsts[i], got_b).astype(jnp.float32) + got_a.astype(jnp.float32))
            z_loc = jnp.zeros(hidden.shape, jnp.float32)
            for s, z in zip(slabs, z_slabs):
                z_loc = lax.dynamic_update_slice_in_dim(z_loc, z, s * slab, axis=2)
            hidden = (hidden.astype(jnp.float32) + z_loc).astype(jnp.bfloat16)
        return hidden

    return jax.shard_map(two_layers, mesh=mesh, in_specs=(P(batch_axes, 'model', None), P(batch_axes), P(None, 'data'), P(None, 'data', 'model'), P(None, 'model', 'data'), P(None, 'model', 'data')), out_specs=P(batch_axes, 'model', None), check_vma=False)
```

```python
import jax
import jax.numpy as jnp
from jax import lax
from jax.experimental import pallas as pl
from jax.experimental.pallas import tpu as pltpu
from jax.sharding import PartitionSpec as P


EPSILON = 1e-6
BOTH = ('data', 'model')


def matmul(lhs, rhs):
    return jnp.dot(lhs, rhs, preferred_element_type=jnp.float32)


def project(h_seq, slab_ids, ours, theirs, total_in, final):
    n_slabs = len(ours)
    rows, cols = h_seq.shape[0], ours[0].shape[1]
    depth = ours[0].shape[0]
    tile, chunk = 512, 512
    tiles = cols // tile
    out_dtype = jnp.bfloat16 if final else jnp.float32

    def kernel(ids_ref, *refs):
        h_refs, w_refs, rest = refs[:n_slabs], refs[n_slabs:3 * n_slabs], refs[3 * n_slabs:]

        def run(w_half):
            @pl.loop(0, rows // chunk)
            def _(step):
                at = pl.ds(pl.multiple_of(step * chunk, chunk), chunk)
                total = matmul(h_refs[0][at, :], w_half[0][...])
                for h_ref, w_ref in zip(h_refs[1:], w_half[1:]):
                    total = total + matmul(h_ref[at, :], w_ref[...])
                if len(rest) == 2:
                    total = total + rest[0][0, at, :]
                rest[-1][0, at, :] = total.astype(out_dtype)

        @pl.when(pl.program_id(0) == 0)
        def _():
            run(w_refs[:n_slabs])

        @pl.when(pl.program_id(0) == 1)
        def _():
            run(w_refs[n_slabs:])

    in_specs = [pl.BlockSpec((rows, depth), lambda p, n, ids, i=i: (0, ids[i])) for i in range(n_slabs)]
    in_specs += [pl.BlockSpec((depth, tile), lambda p, n, ids: (0, jnp.where(p == 0, n, tiles - 1)))] * n_slabs
    in_specs += [pl.BlockSpec((depth, tile), lambda p, n, ids: (0, jnp.where(p == 0, 0, n)))] * n_slabs
    wide = pl.BlockSpec((1, rows, tile), lambda p, n, ids: (p, 0, n))
    args = [h_seq] * n_slabs + list(ours) + list(theirs)
    if total_in is not None:
        in_specs.append(wide)
        args.append(total_in)
    out_shape = jax.ShapeDtypeStruct((2, rows, cols), out_dtype)
    flops = 2 * 2 * n_slabs * rows * depth * cols
    return pl.pallas_call(
        kernel,
        out_shape=out_shape,
        grid_spec=pltpu.PrefetchScalarGridSpec(num_scalar_prefetch=1, grid=(2, tiles), in_specs=in_specs, out_specs=wide),
        cost_estimate=pl.CostEstimate(flops=flops, bytes_accessed=2 * n_slabs * depth * (rows + 2 * cols) + 4 * rows * cols, transcendentals=0),
    )(jnp.stack(slab_ids).astype(jnp.int32), *args)


def mix_out(attn, mlp, ours, theirs):
    _, rows, q_cut = attn.shape
    ff = mlp.shape[2]
    n_slabs = len(ours)
    depth, cols = ours[0].shape
    tile, chunk = 512, 512
    tiles = cols // tile

    def kernel(a_ref, m_ref, *refs):
        w_refs, out_ref = refs[:-1], refs[-1]
        for i in range(n_slabs):
            @pl.when(pl.program_id(0) == i)
            def _(i=i):
                wa_ref, wb_ref = w_refs[i], w_refs[n_slabs + i]

                @pl.loop(0, rows // chunk)
                def _(step):
                    at = pl.ds(pl.multiple_of(step * chunk, chunk), chunk)
                    total = matmul(m_ref[0, at, :], wa_ref[q_cut:, :]) + matmul(m_ref[1, at, :], wb_ref[q_cut:, :])
                    total = total + matmul(a_ref[0, at, :], wa_ref[:q_cut, :]) + matmul(a_ref[1, at, :], wb_ref[:q_cut, :])
                    out_ref[at, :] = total.astype(jnp.bfloat16)

    def w_spec(i):
        return pl.BlockSpec((depth, tile), lambda s, n: (0, jnp.where(s == i, n, jnp.where(s < i, 0, tiles - 1))))

    w_specs = [w_spec(i) for i in range(n_slabs)] * 2
    return pl.pallas_call(
        kernel,
        out_shape=jax.ShapeDtypeStruct((rows, n_slabs * cols), jnp.bfloat16),
        grid=(n_slabs, tiles),
        in_specs=[pl.BlockSpec(attn.shape, lambda s, n: (0, 0, 0)), pl.BlockSpec(mlp.shape, lambda s, n: (0, 0, 0))] + w_specs,
        out_specs=pl.BlockSpec((rows, tile), lambda s, n: (0, s * tiles + n)),
        cost_estimate=pl.CostEstimate(flops=4 * n_slabs * rows * (q_cut + ff) * cols, bytes_accessed=4 * rows * (q_cut + ff) + 4 * n_slabs * depth * cols + 2 * n_slabs * rows * cols, transcendentals=0),
    )(attn, mlp, *ours, *theirs)


def attend(both, core, key_len, head_dim):
    _, rows, _ = both.shape
    chunk = 256

    def kernel(nums_ref, q_ref, k_ref, v_ref, out_ref):
        for step in range(rows // chunk):
            @pl.when(pl.program_id(1) == step)
            def _(step=step):
                seen = (step + 1) * chunk
                scores = lax.dot_general(q_ref[0], k_ref[0, :seen, :], (((1,), (1,)), ((), ())), preferred_element_type=jnp.float32) * head_dim ** -0.5
                q_pos = step * chunk + lax.broadcasted_iota(jnp.int32, scores.shape, 0)
                k_pos = lax.broadcasted_iota(jnp.int32, scores.shape, 1)
                scores = jnp.where((k_pos <= q_pos) & (k_pos < nums_ref[1]), scores, -1e30)
                weights = jnp.exp(scores - jnp.max(scores, axis=-1, keepdims=True))
                norm = jnp.sum(weights, axis=-1, keepdims=True)
                probs = weights / norm
                out = jnp.dot(probs, v_ref[0, :seen, :].astype(jnp.float32), preferred_element_type=jnp.float32)
                out_ref[0] = out.astype(jnp.bfloat16)

    return pl.pallas_call(
        kernel,
        out_shape=jax.ShapeDtypeStruct((2, rows, head_dim), jnp.bfloat16),
        grid_spec=pltpu.PrefetchScalarGridSpec(
            num_scalar_prefetch=1,
            grid=(2, rows // chunk),
            in_specs=[
                pl.BlockSpec((1, chunk, head_dim), lambda j, m, nums: (j, m, 0)),
                pl.BlockSpec((1, rows, head_dim), lambda j, m, nums: (nums[0], 0, 1)),
                pl.BlockSpec((1, rows, head_dim), lambda j, m, nums: (1 - nums[0], 0, 1)),
            ],
            out_specs=pl.BlockSpec((1, chunk, head_dim), lambda j, m, nums: (j, m, 0)),
        ),
        cost_estimate=pl.CostEstimate(flops=8 * rows * rows * head_dim, bytes_accessed=16 * rows * head_dim, transcendentals=2 * rows * rows),
    )(jnp.stack([core, key_len]).astype(jnp.int32), both, both, both)


def normalize(act_f32, gain_row):
    row_mean = jnp.mean(act_f32, axis=-1, keepdims=True)
    centered = act_f32 - row_mean
    row_var = jnp.mean(centered * centered, axis=-1, keepdims=True)
    return (centered * lax.rsqrt(row_var + EPSILON) * gain_row).astype(jnp.bfloat16)


def pair_norm(mine, got_a, got_b, gain, core):
    rows, width = mine.shape

    def kernel(core_ref, mine_ref, a_ref, b_ref, gain_ref, out_ref, norm_ref):
        def emit(at, src_ref):
            val = src_ref[...]
            out_ref[at, :] = val
            norm_ref[at, :] = normalize(val.astype(jnp.float32), gain_ref[...].astype(jnp.float32))

        top, bottom = pl.ds(0, rows), pl.ds(rows, rows)

        @pl.when(core_ref[0] == 0)
        def _():
            emit(top, mine_ref)
            emit(bottom, a_ref)

        @pl.when(core_ref[0] == 1)
        def _():
            emit(top, a_ref)
            emit(bottom, b_ref)

    block = pl.BlockSpec((rows, width), lambda i, c: (0, 0))
    out = pl.BlockSpec((2 * rows, width), lambda i, c: (0, 0))
    return pl.pallas_call(
        kernel,
        out_shape=[jax.ShapeDtypeStruct((2 * rows, width), jnp.bfloat16)] * 2,
        grid_spec=pltpu.PrefetchScalarGridSpec(
            num_scalar_prefetch=1,
            grid=(1,),
            in_specs=[block, block, block, pl.BlockSpec((1, width), lambda i, c: (0, 0))],
            out_specs=[out, out],
        ),
        cost_estimate=pl.CostEstimate(flops=40 * rows * width, bytes_accessed=14 * rows * width, transcendentals=rows),
    )(core.reshape(1).astype(jnp.int32), mine, got_a, got_b, gain.reshape(1, width))


def join_norm(hidden, pairs, others, gain, slab_ids):
    rows, width = hidden.shape
    n_parts = len(pairs)
    slab = width // len(slab_ids)
    chunk = rows // 2

    def kernel(ids_ref, hid_ref, gain_ref, *refs):
        p_refs, o_refs, (out_ref, norm_ref) = refs[:n_parts], refs[n_parts:2 * n_parts], refs[2 * n_parts:]
        for i in range(len(slab_ids)):
            at = pl.ds(pl.multiple_of(ids_ref[i] * slab, slab), slab)
            ours = p_refs[i // 2][:, (i % 2) * slab:(i % 2 + 1) * slab].astype(jnp.float32)
            theirs = o_refs[i // 2][:, (1 - i % 2) * slab:(2 - i % 2) * slab].astype(jnp.float32)
            out_ref[:, at] = (hid_ref[:, at].astype(jnp.float32) + (ours + theirs)).astype(jnp.bfloat16)
        norm_ref[...] = normalize(out_ref[...].astype(jnp.float32), gain_ref[...].astype(jnp.float32))

    wide = pl.BlockSpec((chunk, width), lambda i, ids: (i, 0))
    part = pl.BlockSpec((chunk, 2 * slab), lambda i, ids: (i, 0))
    return pl.pallas_call(
        kernel,
        out_shape=[jax.ShapeDtypeStruct((rows, width), jnp.bfloat16)] * 2,
        grid_spec=pltpu.PrefetchScalarGridSpec(
            num_scalar_prefetch=1,
            grid=(rows // chunk,),
            in_specs=[wide, pl.BlockSpec((1, width), lambda i, ids: (0, 0))] + [part] * (2 * n_parts),
            out_specs=[wide, wide],
        ),
        cost_estimate=pl.CostEstimate(flops=20 * rows * width, bytes_accessed=10 * rows * width, transcendentals=rows),
    )(jnp.stack(slab_ids).astype(jnp.int32), hidden, gain.reshape(1, width), *pairs, *others)


def finish(hidden, residuals, pairs, got_a, got_b, slab_ids, core):
    n_seq = len(hidden)
    rows, width = residuals[0].shape
    slab = width // len(slab_ids)
    n_parts = len(slab_ids) // 2

    def kernel(nums_ref, *refs):
        out_ref = refs[-1]
        even = nums_ref[len(slab_ids)] == 0
        per = 2 + 3 * n_parts
        for b in range(n_seq):
            mine = refs[per * b:per * (b + 1)]
            hid_ref, res_ref, p_refs = mine[0], mine[1], mine[2:2 + n_parts]
            a_refs, b_refs = mine[2 + n_parts:2 + 2 * n_parts], mine[2 + 2 * n_parts:]
            for i in range(len(slab_ids)):
                at = pl.ds(pl.multiple_of(nums_ref[i] * slab, slab), slab)
                cut = slice((i % 2) * slab, (i % 2 + 1) * slab)
                base = jnp.where(even, hid_ref[:, at].astype(jnp.float32), res_ref[:, at].astype(jnp.float32))
                kept = jnp.where(even, p_refs[i // 2][:, cut].astype(jnp.float32), b_refs[i // 2][:, cut].astype(jnp.float32))
                out_ref[b, :, at] = (base + (kept + a_refs[i // 2][:, cut].astype(jnp.float32))).astype(jnp.bfloat16)

    wide = pl.BlockSpec((rows, width), lambda i, n: (0, 0))
    part = pl.BlockSpec((rows, 2 * slab), lambda i, n: (0, 0))
    args = []
    for b in range(n_seq):
        args += [hidden[b], residuals[b], *pairs[b], *got_a[b], *got_b[b]]
    return pl.pallas_call(
        kernel,
        out_shape=jax.ShapeDtypeStruct((n_seq, rows, width), jnp.bfloat16),
        grid_spec=pltpu.PrefetchScalarGridSpec(
            num_scalar_prefetch=1,
            grid=(1,),
            in_specs=([wide, wide] + [part] * (3 * n_parts)) * n_seq,
            out_specs=pl.BlockSpec((n_seq, rows, width), lambda i, n: (0, 0, 0)),
        ),
        cost_estimate=pl.CostEstimate(flops=8 * n_seq * rows * width, bytes_accessed=14 * n_seq * rows * width, transcendentals=0),
    )(jnp.stack([*slab_ids, core]).astype(jnp.int32), *args)


def split_columns(w_in, layer_idx, core, head_dim, q_group, ff_half):
    _, rows, width = w_in.shape
    tile = head_dim
    ff_tiles = ff_half // tile
    n_tiles = width // tile // 2

    def source(n, j):
        gate = q_group + 2 + j * ff_tiles + (n - 2)
        up = q_group + 2 + 2 * ff_tiles + j * ff_tiles + (n - 2 - ff_tiles)
        return jnp.where(n == 0, j, jnp.where(n == 1, q_group + j, jnp.where(n < 2 + ff_tiles, gate, up)))

    def kernel(core_ref, own_ref, other_ref, own_out, other_out):
        own_out[...] = own_ref[0]
        other_out[...] = other_ref[0]

    out = pl.BlockSpec((rows, tile), lambda n, c: (0, n))
    return pl.pallas_call(
        kernel,
        out_shape=[jax.ShapeDtypeStruct((rows, width // 2), w_in.dtype)] * 2,
        grid_spec=pltpu.PrefetchScalarGridSpec(
            num_scalar_prefetch=1,
            grid=(n_tiles,),
            in_specs=[
                pl.BlockSpec((1, rows, tile), lambda n, c: (layer_idx, 0, source(n, c[0]))),
                pl.BlockSpec((1, rows, tile), lambda n, c: (layer_idx, 0, source(n, 1 - c[0]))),
            ],
            out_specs=[out, out],
        ),
        cost_estimate=pl.CostEstimate(flops=rows * width * 8, bytes_accessed=4 * rows * width, transcendentals=0),
    )(core.reshape(1).astype(jnp.int32), w_in, w_in)


def split_rows(w_attn, w_mlp, layer_idx, core):
    _, q_rows, cols = w_attn.shape
    ff = w_mlp.shape[1]
    q_half, ff_half = q_rows // 2, ff // 2
    tile = q_half
    n_tiles = 1 + ff_half // tile

    def kernel(core_ref, own_a, own_m, other_a, other_m, own_out, other_out):
        @pl.when(pl.program_id(0) == 0)
        def _():
            own_out[...] = own_a[0]
            other_out[...] = other_a[0]

        @pl.when(pl.program_id(0) > 0)
        def _():
            own_out[...] = own_m[0]
            other_out[...] = other_m[0]

    def a_spec(flip):
        return pl.BlockSpec((1, tile, cols), lambda n, c: (layer_idx, 1 - c[0] if flip else c[0], 0))

    def m_spec(flip):
        return pl.BlockSpec((1, tile, cols), lambda n, c: (layer_idx, (1 - c[0] if flip else c[0]) * (ff_half // tile) + jnp.maximum(n - 1, 0), 0))

    out = pl.BlockSpec((tile, cols), lambda n, c: (n, 0))
    return pl.pallas_call(
        kernel,
        out_shape=[jax.ShapeDtypeStruct((q_half + ff_half, cols), w_attn.dtype)] * 2,
        grid_spec=pltpu.PrefetchScalarGridSpec(
            num_scalar_prefetch=1,
            grid=(n_tiles,),
            in_specs=[a_spec(False), m_spec(False), a_spec(True), m_spec(True)],
            out_specs=[out, out],
        ),
        cost_estimate=pl.CostEstimate(flops=(q_rows + ff) * cols * 8, bytes_accessed=4 * (q_rows + ff) * cols, transcendentals=0),
    )(core.reshape(1).astype(jnp.int32), w_attn, w_mlp, w_attn, w_mlp)


def solution(mesh):
    n_data, n_model = mesh.shape['data'], mesh.shape['model']
    batch_axes = ('rep', 'data')
    last = n_data - 1

    def table(move):
        pairs = []
        for row in range(n_data):
            for col in range(n_model):
                to = move(row, col)
                if to is not None:
                    pairs.append((row * n_model + col, to[0] * n_model + to[1]))
        return pairs

    core_swap = table(lambda r, m: (r, m ^ 1))
    near_swap = table(lambda r, m: (r ^ 1, m))
    far_swap = table(lambda r, m: (last - r, m))
    spread_a = table(lambda r, m: (r ^ 1, m ^ 1) if m % 2 == 0 else (r, m ^ 1))
    spread_b = table(lambda r, m: None if m % 2 == 0 else (r ^ 1, m))
    collect_a = table(lambda r, m: (r, m ^ 1) if m % 2 == 0 else (r ^ 1, m ^ 1))
    cross = table(lambda r, m: (r ^ 1, m ^ 1))
    lanes = [list(range(0, n_model, 2)), list(range(1, n_model, 2))]

    def send(val, pairs):
        return lax.ppermute(val, BOTH, pairs)

    def two_layers(x_loc, len_loc, gain_loc, w_in_loc, w_attn_loc, w_mlp_loc):
        n_layers, slab, block_in = w_in_loc.shape
        attn_width = w_attn_loc.shape[1]
        ff_local = w_mlp_loc.shape[1]
        head_dim = (block_in - attn_width - 2 * ff_local) // 2
        q_group = attn_width // head_dim
        batch_loc, seq_loc = x_loc.shape[0], x_loc.shape[1]
        ff_half = ff_local // 2
        row = lax.axis_index('data')
        core = lax.rem(lax.axis_index('model'), 2)
        even = core == 0
        wanted = lax.rem((row + 1) // 2, 2)
        mine_wanted = wanted == core
        slabs = (row, row ^ 1, last - row, (last - row) ^ 1)

        work_lens = jnp.where(even, len_loc, send(len_loc, near_swap))
        gain_all = lax.all_gather(gain_loc, 'data', axis=1, tiled=True)

        def pieces(keep_half, give_half):
            other = send(give_half, core_swap)
            keep = jnp.where(mine_wanted, keep_half, other)
            give = jnp.where(mine_wanted, other, keep_half)
            near = send(give, near_swap)
            far = send(keep, far_swap)
            far_near = send(near, far_swap)
            ours = (keep, near, far, far_near)
            theirs = tuple(send(p, core_swap) for p in ours)
            return ours, theirs

        w_pieces = []
        for layer_idx in range(n_layers):
            ins = pieces(*split_columns(w_in_loc, layer_idx, core, head_dim, q_group, ff_half))
            outs = pieces(*split_rows(w_attn_loc, w_mlp_loc, layer_idx, core))
            w_pieces.append((ins, outs))

        hidden, normed = [], []
        for b in range(batch_loc):
            mine = x_loc[b]
            got_a = send(mine, spread_a)
            got_b = send(mine, spread_b)
            hid, norm = pair_norm(mine, got_a, got_b, gain_all[0], core)
            hidden.append(hid)
            normed.append(norm)

        def swap_slabs(val):
            return jnp.concatenate([val[:, slab:], val[:, :slab]], axis=1)

        ends = ([], [], [], [])
        for layer_idx in range(n_layers):
            ins, outs = w_pieces[layer_idx]
            is_last = layer_idx == n_layers - 1
            h_seqs = [lax.all_gather(n, 'model', axis=0, tiled=True, axis_index_groups=lanes) for n in normed]
            normed = []
            totals = []
            for b in range(batch_loc):
                if layer_idx == 0:
                    totals.append(project(h_seqs[b], slabs[:3], ins[0][:3], ins[1][:3], None, False))
            new_hidden = []
            for b in range(batch_loc):
                if layer_idx == 0:
                    both = project(h_seqs[b], slabs[3:], ins[0][3:], ins[1][3:], totals[b], True)
                else:
                    both = project(h_seqs[b], slabs, ins[0], ins[1], None, True)
                ff_at = attn_width // 2 + head_dim
                attn = attend(both, core, work_lens[b], head_dim)
                gate, up = both[:, :, ff_at:ff_at + ff_half], both[:, :, ff_at + ff_half:]
                mlp = (jax.nn.silu(gate.astype(jnp.float32)) * up.astype(jnp.float32)).astype(jnp.bfloat16)
                pairs, got_a, got_b, others = [], [], [], []
                for s in range(2):
                    part = mix_out(attn, mlp, outs[0][2 * s:2 * s + 2], outs[1][2 * s:2 * s + 2])
                    pair = lax.psum_scatter(part, 'model', scatter_dimension=0, tiled=True, axis_index_groups=lanes)
                    pairs.append(pair)
                    if is_last:
                        first, second = pair[:seq_loc], pair[seq_loc:]
                        got_a.append(send(jnp.where(even, second, swap_slabs(first)), collect_a))
                        got_b.append(send(swap_slabs(second), spread_b))
                    else:
                        others.append(send(pair, cross))
                if is_last:
                    for kept, val in zip(ends, (send(hidden[b][seq_loc:], core_swap), pairs, got_a, got_b)):
                        kept.append(val)
                else:
                    hid, norm = join_norm(hidden[b], pairs, others, gain_all[layer_idx + 1], slabs)
                    new_hidden.append(hid)
                    normed.append(norm)
            if not is_last:
                hidden = new_hidden
        return finish(hidden, *ends, slabs, core)

    return jax.shard_map(two_layers, mesh=mesh, in_specs=(P(batch_axes, 'model', None), P(batch_axes), P(None, 'data'), P(None, 'data', 'model'), P(None, 'model', 'data'), P(None, 'model', 'data')), out_specs=P(batch_axes, 'model', None), check_vma=False)
```

```python
import jax
import jax.numpy as jnp
from jax import lax
from jax.experimental import pallas as pl
from jax.experimental.pallas import tpu as pltpu
from jax.sharding import PartitionSpec as P


EPSILON = 1e-6
BOTH = ('data', 'model')


def matmul(lhs, rhs):
    return jnp.dot(lhs, rhs, preferred_element_type=jnp.float32)


def project(h_seq, slab_ids, ours, theirs, total_in, final):
    n_slabs = len(ours)
    rows, cols = h_seq.shape[0], ours[0].shape[1]
    depth = ours[0].shape[0]
    tile, chunk = 512, 1024
    tiles = cols // tile
    out_dtype = jnp.bfloat16 if final else jnp.float32

    def kernel(ids_ref, *refs):
        h_refs, w_refs, rest = refs[:n_slabs], refs[n_slabs:3 * n_slabs], refs[3 * n_slabs:]

        def run(w_half):
            @pl.loop(0, rows // chunk)
            def _(step):
                at = pl.ds(pl.multiple_of(step * chunk, chunk), chunk)
                lhs = jnp.concatenate([h_ref[at, :] for h_ref in h_refs], axis=1)
                rhs = jnp.concatenate([w_ref[...] for w_ref in w_half], axis=0)
                total = matmul(lhs, rhs)
                if len(rest) == 2:
                    total = total + rest[0][0, at, :]
                rest[-1][0, at, :] = total.astype(out_dtype)

        @pl.when(pl.program_id(0) == 0)
        def _():
            run(w_refs[:n_slabs])

        @pl.when(pl.program_id(0) == 1)
        def _():
            run(w_refs[n_slabs:])

    in_specs = [pl.BlockSpec((rows, depth), lambda p, n, ids, i=i: (0, ids[i])) for i in range(n_slabs)]
    in_specs += [pl.BlockSpec((depth, tile), lambda p, n, ids: (0, jnp.where(p == 0, n, tiles - 1)))] * n_slabs
    in_specs += [pl.BlockSpec((depth, tile), lambda p, n, ids: (0, jnp.where(p == 0, 0, n)))] * n_slabs
    wide = pl.BlockSpec((1, rows, tile), lambda p, n, ids: (p, 0, n))
    args = [h_seq] * n_slabs + list(ours) + list(theirs)
    if total_in is not None:
        in_specs.append(wide)
        args.append(total_in)
    out_shape = jax.ShapeDtypeStruct((2, rows, cols), out_dtype)
    flops = 2 * 2 * n_slabs * rows * depth * cols
    return pl.pallas_call(
        kernel,
        out_shape=out_shape,
        grid_spec=pltpu.PrefetchScalarGridSpec(num_scalar_prefetch=1, grid=(2, tiles), in_specs=in_specs, out_specs=wide),
        cost_estimate=pl.CostEstimate(flops=flops, bytes_accessed=2 * n_slabs * depth * (rows + 2 * cols) + 4 * rows * cols, transcendentals=0),
    )(jnp.stack(slab_ids).astype(jnp.int32), *args)


def mix_out(attn, mlp, ours, theirs):
    _, rows, q_cut = attn.shape
    ff = mlp.shape[2]
    n_slabs = len(ours)
    depth, cols = ours[0].shape
    tile, chunk = 512, 1024
    tiles = cols // tile

    def kernel(a_ref, m_ref, *refs):
        w_refs, out_ref = refs[:-1], refs[-1]
        for i in range(n_slabs):
            @pl.when(pl.program_id(0) == i)
            def _(i=i):
                wa_ref, wb_ref = w_refs[i], w_refs[n_slabs + i]

                @pl.loop(0, rows // chunk)
                def _(step):
                    at = pl.ds(pl.multiple_of(step * chunk, chunk), chunk)
                    lhs = jnp.concatenate([a_ref[0, at, :], m_ref[0, at, :], a_ref[1, at, :], m_ref[1, at, :]], axis=1)
                    rhs = jnp.concatenate([wa_ref[...], wb_ref[...]], axis=0)
                    out_ref[at, :] = matmul(lhs, rhs).astype(jnp.bfloat16)

    def w_spec(i):
        return pl.BlockSpec((depth, tile), lambda s, n: (0, jnp.where(s == i, n, jnp.where(s < i, 0, tiles - 1))))

    w_specs = [w_spec(i) for i in range(n_slabs)] * 2
    return pl.pallas_call(
        kernel,
        out_shape=jax.ShapeDtypeStruct((rows, n_slabs * cols), jnp.bfloat16),
        grid=(n_slabs, tiles),
        in_specs=[pl.BlockSpec(attn.shape, lambda s, n: (0, 0, 0)), pl.BlockSpec(mlp.shape, lambda s, n: (0, 0, 0))] + w_specs,
        out_specs=pl.BlockSpec((rows, tile), lambda s, n: (0, s * tiles + n)),
        cost_estimate=pl.CostEstimate(flops=4 * n_slabs * rows * (q_cut + ff) * cols, bytes_accessed=4 * rows * (q_cut + ff) + 4 * n_slabs * depth * cols + 2 * n_slabs * rows * cols, transcendentals=0),
    )(attn, mlp, *ours, *theirs)


def attend(both, core, key_len, head_dim):
    _, rows, _ = both.shape
    chunk = 256

    def kernel(nums_ref, q_ref, k_ref, v_ref, out_ref):
        for step in range(rows // chunk):
            @pl.when(pl.program_id(1) == step)
            def _(step=step):
                seen = (step + 1) * chunk
                scores = lax.dot_general(q_ref[0], k_ref[0, :seen, :], (((1,), (1,)), ((), ())), preferred_element_type=jnp.float32) * head_dim ** -0.5
                q_pos = step * chunk + lax.broadcasted_iota(jnp.int32, scores.shape, 0)
                k_pos = lax.broadcasted_iota(jnp.int32, scores.shape, 1)
                scores = jnp.where((k_pos <= q_pos) & (k_pos < nums_ref[1]), scores, -1e30)
                weights = jnp.exp(scores - jnp.max(scores, axis=-1, keepdims=True))
                norm = jnp.sum(weights, axis=-1, keepdims=True)
                probs = weights / norm
                out = jnp.dot(probs, v_ref[0, :seen, :].astype(jnp.float32), preferred_element_type=jnp.float32)
                out_ref[0] = out.astype(jnp.bfloat16)

    return pl.pallas_call(
        kernel,
        out_shape=jax.ShapeDtypeStruct((2, rows, head_dim), jnp.bfloat16),
        grid_spec=pltpu.PrefetchScalarGridSpec(
            num_scalar_prefetch=1,
            grid=(2, rows // chunk),
            in_specs=[
                pl.BlockSpec((1, chunk, head_dim), lambda j, m, nums: (j, m, 0)),
                pl.BlockSpec((1, rows, head_dim), lambda j, m, nums: (nums[0], 0, 1)),
                pl.BlockSpec((1, rows, head_dim), lambda j, m, nums: (1 - nums[0], 0, 1)),
            ],
            out_specs=pl.BlockSpec((1, chunk, head_dim), lambda j, m, nums: (j, m, 0)),
        ),
        cost_estimate=pl.CostEstimate(flops=8 * rows * rows * head_dim, bytes_accessed=16 * rows * head_dim, transcendentals=2 * rows * rows),
    )(jnp.stack([core, key_len]).astype(jnp.int32), both, both, both)


def normalize(act_f32, gain_row):
    row_mean = jnp.mean(act_f32, axis=-1, keepdims=True)
    centered = act_f32 - row_mean
    row_var = jnp.mean(centered * centered, axis=-1, keepdims=True)
    return (centered * lax.rsqrt(row_var + EPSILON) * gain_row).astype(jnp.bfloat16)


def pair_norm(mine, got_a, got_b, gain, core):
    rows, width = mine.shape

    def kernel(core_ref, mine_ref, a_ref, b_ref, gain_ref, out_ref, norm_ref):
        def emit(at, src_ref):
            val = src_ref[...]
            out_ref[at, :] = val
            norm_ref[at, :] = normalize(val.astype(jnp.float32), gain_ref[...].astype(jnp.float32))

        top, bottom = pl.ds(0, rows), pl.ds(rows, rows)

        @pl.when(core_ref[0] == 0)
        def _():
            emit(top, mine_ref)
            emit(bottom, a_ref)

        @pl.when(core_ref[0] == 1)
        def _():
            emit(top, a_ref)
            emit(bottom, b_ref)

    block = pl.BlockSpec((rows, width), lambda i, c: (0, 0))
    out = pl.BlockSpec((2 * rows, width), lambda i, c: (0, 0))
    return pl.pallas_call(
        kernel,
        out_shape=[jax.ShapeDtypeStruct((2 * rows, width), jnp.bfloat16)] * 2,
        grid_spec=pltpu.PrefetchScalarGridSpec(
            num_scalar_prefetch=1,
            grid=(1,),
            in_specs=[block, block, block, pl.BlockSpec((1, width), lambda i, c: (0, 0))],
            out_specs=[out, out],
        ),
        cost_estimate=pl.CostEstimate(flops=40 * rows * width, bytes_accessed=14 * rows * width, transcendentals=rows),
    )(core.reshape(1).astype(jnp.int32), mine, got_a, got_b, gain.reshape(1, width))


def join_norm(hidden, pairs, others, gain, slab_ids):
    rows, width = hidden.shape
    n_parts = len(pairs)
    slab = width // len(slab_ids)
    chunk = rows // 2

    def kernel(ids_ref, hid_ref, gain_ref, *refs):
        p_refs, o_refs, (out_ref, norm_ref) = refs[:n_parts], refs[n_parts:2 * n_parts], refs[2 * n_parts:]
        for i in range(len(slab_ids)):
            at = pl.ds(pl.multiple_of(ids_ref[i] * slab, slab), slab)
            ours = p_refs[i // 2][:, (i % 2) * slab:(i % 2 + 1) * slab].astype(jnp.float32)
            theirs = o_refs[i // 2][:, (1 - i % 2) * slab:(2 - i % 2) * slab].astype(jnp.float32)
            out_ref[:, at] = (hid_ref[:, at].astype(jnp.float32) + (ours + theirs)).astype(jnp.bfloat16)
        norm_ref[...] = normalize(out_ref[...].astype(jnp.float32), gain_ref[...].astype(jnp.float32))

    wide = pl.BlockSpec((chunk, width), lambda i, ids: (i, 0))
    part = pl.BlockSpec((chunk, 2 * slab), lambda i, ids: (i, 0))
    return pl.pallas_call(
        kernel,
        out_shape=[jax.ShapeDtypeStruct((rows, width), jnp.bfloat16)] * 2,
        grid_spec=pltpu.PrefetchScalarGridSpec(
            num_scalar_prefetch=1,
            grid=(rows // chunk,),
            in_specs=[wide, pl.BlockSpec((1, width), lambda i, ids: (0, 0))] + [part] * (2 * n_parts),
            out_specs=[wide, wide],
        ),
        cost_estimate=pl.CostEstimate(flops=20 * rows * width, bytes_accessed=10 * rows * width, transcendentals=rows),
    )(jnp.stack(slab_ids).astype(jnp.int32), hidden, gain.reshape(1, width), *pairs, *others)


def finish(hidden, residuals, pairs, got_a, got_b, slab_ids, core):
    n_seq = len(hidden)
    rows, width = residuals[0].shape
    slab = width // len(slab_ids)
    n_parts = len(slab_ids) // 2

    def kernel(nums_ref, *refs):
        out_ref = refs[-1]
        even = nums_ref[len(slab_ids)] == 0
        per = 2 + 3 * n_parts
        for b in range(n_seq):
            mine = refs[per * b:per * (b + 1)]
            hid_ref, res_ref, p_refs = mine[0], mine[1], mine[2:2 + n_parts]
            a_refs, b_refs = mine[2 + n_parts:2 + 2 * n_parts], mine[2 + 2 * n_parts:]
            for i in range(len(slab_ids)):
                at = pl.ds(pl.multiple_of(nums_ref[i] * slab, slab), slab)
                cut = slice((i % 2) * slab, (i % 2 + 1) * slab)
                base = jnp.where(even, hid_ref[:, at].astype(jnp.float32), res_ref[:, at].astype(jnp.float32))
                kept = jnp.where(even, p_refs[i // 2][:, cut].astype(jnp.float32), b_refs[i // 2][:, cut].astype(jnp.float32))
                out_ref[b, :, at] = (base + (kept + a_refs[i // 2][:, cut].astype(jnp.float32))).astype(jnp.bfloat16)

    wide = pl.BlockSpec((rows, width), lambda i, n: (0, 0))
    part = pl.BlockSpec((rows, 2 * slab), lambda i, n: (0, 0))
    args = []
    for b in range(n_seq):
        args += [hidden[b], residuals[b], *pairs[b], *got_a[b], *got_b[b]]
    return pl.pallas_call(
        kernel,
        out_shape=jax.ShapeDtypeStruct((n_seq, rows, width), jnp.bfloat16),
        grid_spec=pltpu.PrefetchScalarGridSpec(
            num_scalar_prefetch=1,
            grid=(1,),
            in_specs=([wide, wide] + [part] * (3 * n_parts)) * n_seq,
            out_specs=pl.BlockSpec((n_seq, rows, width), lambda i, n: (0, 0, 0)),
        ),
        cost_estimate=pl.CostEstimate(flops=8 * n_seq * rows * width, bytes_accessed=14 * n_seq * rows * width, transcendentals=0),
    )(jnp.stack([*slab_ids, core]).astype(jnp.int32), *args)


def split_columns(w_in, layer_idx, core, head_dim, q_group, ff_half):
    _, rows, width = w_in.shape
    tile = head_dim
    ff_tiles = ff_half // tile
    n_tiles = width // tile // 2

    def source(n, j):
        gate = q_group + 2 + j * ff_tiles + (n - 2)
        up = q_group + 2 + 2 * ff_tiles + j * ff_tiles + (n - 2 - ff_tiles)
        return jnp.where(n == 0, j, jnp.where(n == 1, q_group + j, jnp.where(n < 2 + ff_tiles, gate, up)))

    def kernel(core_ref, own_ref, other_ref, own_out, other_out):
        own_out[...] = own_ref[0]
        other_out[...] = other_ref[0]

    out = pl.BlockSpec((rows, tile), lambda n, c: (0, n))
    return pl.pallas_call(
        kernel,
        out_shape=[jax.ShapeDtypeStruct((rows, width // 2), w_in.dtype)] * 2,
        grid_spec=pltpu.PrefetchScalarGridSpec(
            num_scalar_prefetch=1,
            grid=(n_tiles,),
            in_specs=[
                pl.BlockSpec((1, rows, tile), lambda n, c: (layer_idx, 0, source(n, c[0]))),
                pl.BlockSpec((1, rows, tile), lambda n, c: (layer_idx, 0, source(n, 1 - c[0]))),
            ],
            out_specs=[out, out],
        ),
        cost_estimate=pl.CostEstimate(flops=rows * width * 8, bytes_accessed=4 * rows * width, transcendentals=0),
    )(core.reshape(1).astype(jnp.int32), w_in, w_in)


def split_rows(w_attn, w_mlp, layer_idx, core):
    _, q_rows, cols = w_attn.shape
    ff = w_mlp.shape[1]
    q_half, ff_half = q_rows // 2, ff // 2
    tile = q_half
    n_tiles = 1 + ff_half // tile

    def kernel(core_ref, own_a, own_m, other_a, other_m, own_out, other_out):
        @pl.when(pl.program_id(0) == 0)
        def _():
            own_out[...] = own_a[0]
            other_out[...] = other_a[0]

        @pl.when(pl.program_id(0) > 0)
        def _():
            own_out[...] = own_m[0]
            other_out[...] = other_m[0]

    def a_spec(flip):
        return pl.BlockSpec((1, tile, cols), lambda n, c: (layer_idx, 1 - c[0] if flip else c[0], 0))

    def m_spec(flip):
        return pl.BlockSpec((1, tile, cols), lambda n, c: (layer_idx, (1 - c[0] if flip else c[0]) * (ff_half // tile) + jnp.maximum(n - 1, 0), 0))

    out = pl.BlockSpec((tile, cols), lambda n, c: (n, 0))
    return pl.pallas_call(
        kernel,
        out_shape=[jax.ShapeDtypeStruct((q_half + ff_half, cols), w_attn.dtype)] * 2,
        grid_spec=pltpu.PrefetchScalarGridSpec(
            num_scalar_prefetch=1,
            grid=(n_tiles,),
            in_specs=[a_spec(False), m_spec(False), a_spec(True), m_spec(True)],
            out_specs=[out, out],
        ),
        cost_estimate=pl.CostEstimate(flops=(q_rows + ff) * cols * 8, bytes_accessed=4 * (q_rows + ff) * cols, transcendentals=0),
    )(core.reshape(1).astype(jnp.int32), w_attn, w_mlp, w_attn, w_mlp)


def solution(mesh):
    n_data, n_model = mesh.shape['data'], mesh.shape['model']
    batch_axes = ('rep', 'data')
    last = n_data - 1

    def table(move):
        pairs = []
        for row in range(n_data):
            for col in range(n_model):
                to = move(row, col)
                if to is not None:
                    pairs.append((row * n_model + col, to[0] * n_model + to[1]))
        return pairs

    core_swap = table(lambda r, m: (r, m ^ 1))
    near_swap = table(lambda r, m: (r ^ 1, m))
    far_swap = table(lambda r, m: (last - r, m))
    spread_a = table(lambda r, m: (r ^ 1, m ^ 1) if m % 2 == 0 else (r, m ^ 1))
    spread_b = table(lambda r, m: None if m % 2 == 0 else (r ^ 1, m))
    collect_a = table(lambda r, m: (r, m ^ 1) if m % 2 == 0 else (r ^ 1, m ^ 1))
    cross = table(lambda r, m: (r ^ 1, m ^ 1))
    lanes = [list(range(0, n_model, 2)), list(range(1, n_model, 2))]

    def send(val, pairs):
        return lax.ppermute(val, BOTH, pairs)

    def two_layers(x_loc, len_loc, gain_loc, w_in_loc, w_attn_loc, w_mlp_loc):
        n_layers, slab, block_in = w_in_loc.shape
        attn_width = w_attn_loc.shape[1]
        ff_local = w_mlp_loc.shape[1]
        head_dim = (block_in - attn_width - 2 * ff_local) // 2
        q_group = attn_width // head_dim
        batch_loc, seq_loc = x_loc.shape[0], x_loc.shape[1]
        ff_half = ff_local // 2
        row = lax.axis_index('data')
        core = lax.rem(lax.axis_index('model'), 2)
        even = core == 0
        wanted = lax.rem((row + 1) // 2, 2)
        mine_wanted = wanted == core
        slabs = (row, row ^ 1, last - row, (last - row) ^ 1)

        work_lens = jnp.where(even, len_loc, send(len_loc, near_swap))
        gain_near = send(gain_loc, near_swap)
        gain_far = send(gain_loc, far_swap)
        gain_fn = send(gain_near, far_swap)
        gain_all = jnp.zeros((n_layers, n_data * slab), gain_loc.dtype)
        for s, g in zip(slabs, (gain_loc, gain_near, gain_far, gain_fn)):
            gain_all = lax.dynamic_update_slice_in_dim(gain_all, g, s * slab, axis=1)

        def pieces(keep_half, give_half):
            other = send(give_half, core_swap)
            keep = jnp.where(mine_wanted, keep_half, other)
            give = jnp.where(mine_wanted, other, keep_half)
            near = send(give, near_swap)
            far = send(keep, far_swap)
            far_near = send(near, far_swap)
            ours = (keep, near, far, far_near)
            theirs = tuple(send(p, core_swap) for p in ours)
            return ours, theirs

        w_pieces = []
        for layer_idx in range(n_layers):
            ins = pieces(*split_columns(w_in_loc, layer_idx, core, head_dim, q_group, ff_half))
            outs = pieces(*split_rows(w_attn_loc, w_mlp_loc, layer_idx, core))
            w_pieces.append((ins, outs))

        hidden, normed = [], []
        for b in range(batch_loc):
            mine = x_loc[b]
            got_a = send(mine, spread_a)
            got_b = send(mine, spread_b)
            hid, norm = pair_norm(mine, got_a, got_b, gain_all[0], core)
            hidden.append(hid)
            normed.append(norm)

        def swap_slabs(val):
            return jnp.concatenate([val[:, slab:], val[:, :slab]], axis=1)

        ends = ([], [], [], [])
        for layer_idx in range(n_layers):
            ins, outs = w_pieces[layer_idx]
            is_last = layer_idx == n_layers - 1
            h_seqs = [lax.all_gather(n, 'model', axis=0, tiled=True, axis_index_groups=lanes) for n in normed]
            normed = []
            totals = []
            for b in range(batch_loc):
                if layer_idx == 0:
                    totals.append(project(h_seqs[b], slabs[:3], ins[0][:3], ins[1][:3], None, False))
            new_hidden = []
            for b in range(batch_loc):
                if layer_idx == 0:
                    both = project(h_seqs[b], slabs[3:], ins[0][3:], ins[1][3:], totals[b], True)
                else:
                    both = project(h_seqs[b], slabs, ins[0], ins[1], None, True)
                ff_at = attn_width // 2 + head_dim
                attn = attend(both, core, work_lens[b], head_dim)
                gate, up = both[:, :, ff_at:ff_at + ff_half], both[:, :, ff_at + ff_half:]
                mlp = (jax.nn.silu(gate.astype(jnp.float32)) * up.astype(jnp.float32)).astype(jnp.bfloat16)
                pairs, got_a, got_b, others = [], [], [], []
                for s in range(2):
                    part = mix_out(attn, mlp, outs[0][2 * s:2 * s + 2], outs[1][2 * s:2 * s + 2])
                    pair = lax.psum_scatter(part, 'model', scatter_dimension=0, tiled=True, axis_index_groups=lanes)
                    pairs.append(pair)
                    if is_last:
                        first, second = pair[:seq_loc], pair[seq_loc:]
                        got_a.append(send(jnp.where(even, second, swap_slabs(first)), collect_a))
                        got_b.append(send(swap_slabs(second), spread_b))
                    else:
                        others.append(send(pair, cross))
                if is_last:
                    for kept, val in zip(ends, (send(hidden[b][seq_loc:], core_swap), pairs, got_a, got_b)):
                        kept.append(val)
                else:
                    hid, norm = join_norm(hidden[b], pairs, others, gain_all[layer_idx + 1], slabs)
                    new_hidden.append(hid)
                    normed.append(norm)
            if not is_last:
                hidden = new_hidden
        return finish(hidden, *ends, slabs, core)

    return jax.shard_map(two_layers, mesh=mesh, in_specs=(P(batch_axes, 'model', None), P(batch_axes), P(None, 'data'), P(None, 'data', 'model'), P(None, 'model', 'data'), P(None, 'model', 'data')), out_specs=P(batch_axes, 'model', None), check_vma=False)
```
